32 devices in a mesh: tm: 8 (over z, x), pair: 4 (over y, core).
Axes of the slice: x: 2, y: 2, z: 4, core: 2. Of those that a mesh axis runs over, the one named last changes fastest.
Arguments:
- voltages: bfloat16 [2, 32, 262144], P(None, 'pair', 'tm'), may hold values from -3 to 3
- delays: int32 [32, 32], P('pair', 'tm'), may hold values from 0 to 49152, as said below
- phase_model: float32 [32, 8192], replicated, may hold values from -3.140625 to 3.140625
- phase_bins: int32 [32], P('tm'), may hold values from 0 to 31
- assignment: int32 [16], P('pair'), may hold values from 0 to 15, each once
Outputs:
- visibility: float32 [32, 16, 2, 64, 128], P('tm', 'pair')
The draws below stay inside these ranges and needn't reach their ends.
Inputs may be any that keep to these rules, and one draw needn't show every extreme that they name: `delays`: delay of each station in each recording block of 1 frames; both 0 and 49152 occur in every draw. `assignment`: each of the 16 station-pair blocks occurs once.
All inputs are finite; a program needn't handle non-finite values.
Results may differ from the reference program's by a relative error of at most 0.0085.
Values may be sent and summed in bfloat16 or wider, within the bound.
A program may use at most 128 MiB of HBM per device.

```python
import math
import jax
import jax.numpy as jnp
from jax import lax

NCHAN = 8192
STATIONS = 32
GROUP_ST = 8
RADIX_A = 16
CHAVG = 64
BINS = 32
FB = 1
NGRP = 4
NBLK = 16
OUTCH = 128
FRAMES = 32
BLOCKS = 32
SAMPLES = 262144
DELAY_MAX = 49152


def draw_delays(key, part):
    entries = STATIONS * BLOCKS
    values = jax.random.randint(jax.random.fold_in(key, 11), (entries,), 0, DELAY_MAX + 1, dtype=jnp.int32)
    highest = jax.random.randint(jax.random.fold_in(key, 12), (), 0, entries, dtype=jnp.int32)
    advance = jax.random.randint(jax.random.fold_in(key, 13), (), 1, entries, dtype=jnp.int32)
    lowest = (highest + advance) % entries
    places = jnp.arange(entries, dtype=jnp.int32)
    values = jnp.where(places == highest, DELAY_MAX, values)
    values = jnp.where(places == lowest, 0, values)
    return values.reshape(STATIONS, BLOCKS).astype(jnp.int32)


def touch_ends(values, rng, low, largest):
    extent = values.shape
    spot = [jax.random.randint(jax.random.fold_in(rng, axis), (), 0, extent[axis]) for axis in range(len(extent))]
    values = values.at[tuple(spot)].set(low)
    longest = extent.index(max(extent))
    spot[longest] = (spot[longest] + 1) % extent[longest]
    return values.at[tuple(spot)].set(largest)


def block_levels(rng, extent, split, smallest, high):
    loudness, own = 1.0, jax.random.fold_in(rng, 6)
    for position, shards_of in split:
        steps = jnp.exp(jax.random.uniform(jax.random.fold_in(own, position), (shards_of,), jnp.float32, smallest / len(split), high / len(split)))
        loudness = loudness * jnp.repeat(steps, extent[position] // shards_of).reshape([-1 if axis == position else 1 for axis in range(len(extent))])
    return loudness


def gaussian(rng, extent, deviation, limit, split=(), kind=jnp.bfloat16):
    values = jax.random.normal(rng, extent, jnp.float32) * deviation
    if len(split) > 0:
        values = block_levels(rng, extent, split, -0.22, 0.18) * values
    return jnp.clip(values, min=-limit, max=limit).astype(kind)


def setup_inputs(seed: int = 0) -> dict:
    keys = jax.random.split(jax.random.key(seed), 6)
    voltages = gaussian(keys[0], (2, STATIONS, SAMPLES), 0.5, 3.0, ((1, 4), (2, 8)))
    delays = draw_delays(jax.random.fold_in(keys[5], 71), 0)
    phase_model = jnp.clip(jax.random.uniform(keys[2], (STATIONS, NCHAN), jnp.float32, -3.140625, 3.140625), -3.140625, 3.140625)
    phase_bins = touch_ends(jax.random.randint(keys[3], (FRAMES,), 0, BINS), jax.random.fold_in(keys[3], 1), 0, BINS - 1).astype(jnp.int32)
    assignment = jax.random.permutation(keys[4], NBLK).astype(jnp.int32)
    return {"voltages": voltages, "delays": delays, "phase_model": phase_model, "phase_bins": phase_bins, "assignment": assignment}


def dft_tables(radix_small, radix_large):
    index_small = jnp.arange(radix_small, dtype=jnp.int32)
    index_large = jnp.arange(radix_large, dtype=jnp.int32)
    small_turns = index_small[:, None] * index_small[None, :] % radix_small
    small_angle = small_turns.astype(jnp.float32) * (2.0 * math.pi / radix_small)
    small_scale = 1.0 / math.sqrt(radix_small)
    small_cos = (jnp.cos(small_angle) * small_scale).astype(jnp.bfloat16)
    small_sin = (jnp.sin(small_angle) * small_scale).astype(jnp.bfloat16)
    twist_turns = index_small[:, None] * index_large[None, :]
    twist_angle = twist_turns.astype(jnp.float32) * (2.0 * math.pi / (radix_small * radix_large))
    twist_cos = jnp.cos(twist_angle)
    twist_sin = jnp.sin(twist_angle)
    large_turns = index_large[:, None] * index_large[None, :] % radix_large
    large_angle = large_turns.astype(jnp.float32) * (2.0 * math.pi / radix_large)
    large_scale = 1.0 / math.sqrt(radix_large)
    large_cos = (jnp.cos(large_angle) * large_scale).astype(jnp.bfloat16)
    large_sin = (jnp.sin(large_angle) * large_scale).astype(jnp.bfloat16)
    return (small_cos, small_sin, twist_cos, twist_sin, large_cos, large_sin)

def reference(voltages, delays, phase_model, phase_bins, assignment):
    radix_large = NCHAN // RADIX_A
    group_width = radix_large // OUTCH
    highest = lax.Precision.HIGHEST
    small_cos, small_sin, twist_cos, twist_sin, large_cos, large_sin = dft_tables(RADIX_A, radix_large)
    small_cos = small_cos.astype(jnp.float32)
    small_sin = small_sin.astype(jnp.float32)
    large_cos = large_cos.astype(jnp.float32)
    large_sin = large_sin.astype(jnp.float32)
    padded = jnp.pad(voltages, ((0, 0), (0, 0), (0, DELAY_MAX)))
    angles = phase_model.reshape(STATIONS, radix_large, RADIX_A).transpose(0, 2, 1)
    phase_cos = jnp.cos(angles)
    phase_sin = jnp.sin(angles)

    def cut(series, offset):
        return lax.dynamic_slice_in_dim(series, offset, NCHAN, 1)

    def frame_products(frame):
        offsets = (frame * NCHAN + delays[:, frame // FB]).astype(jnp.int32)
        window = jax.vmap(cut, in_axes=(1, 0), out_axes=1)(padded, offsets)
        samples = window.astype(jnp.float32).reshape(2, STATIONS, RADIX_A, radix_large)
        first_real = jnp.einsum('kn,snm->skm', small_cos, samples[0], precision=highest) + jnp.einsum('kn,snm->skm', small_sin, samples[1], precision=highest)
        first_imag = jnp.einsum('kn,snm->skm', small_cos, samples[1], precision=highest) - jnp.einsum('kn,snm->skm', small_sin, samples[0], precision=highest)
        turned = jnp.stack([first_real * twist_cos + first_imag * twist_sin, first_imag * twist_cos - first_real * twist_sin]).astype(jnp.bfloat16)
        turned = lax.optimization_barrier(turned).astype(jnp.float32)
        chan_real = jnp.einsum('skm,mc->skc', turned[0], large_cos, precision=highest) + jnp.einsum('skm,mc->skc', turned[1], large_sin, precision=highest)
        chan_imag = jnp.einsum('skm,mc->skc', turned[1], large_cos, precision=highest) - jnp.einsum('skm,mc->skc', turned[0], large_sin, precision=highest)
        spectra = jnp.stack([chan_real * phase_cos - chan_imag * phase_sin, chan_real * phase_sin + chan_imag * phase_cos]).astype(jnp.bfloat16)
        spectra = lax.optimization_barrier(spectra).astype(jnp.float32)
        grouped = spectra.reshape(2, STATIONS, RADIX_A, OUTCH, group_width)
        gram_terms = jnp.einsum('riagq,sjagq->rsgij', grouped, grouped, precision=highest)
        real_part = gram_terms[0, 0] + gram_terms[1, 1]
        imag_part = gram_terms[1, 0] - gram_terms[0, 1]
        return jnp.stack([real_part, imag_part]) * (1.0 / CHAVG)
    products = lax.map(frame_products, jnp.arange(FRAMES, dtype=jnp.int32))
    onehot = (phase_bins[:, None] == jnp.arange(BINS, dtype=jnp.int32)[None, :]).astype(jnp.float32)
    binned = jnp.dot(onehot.T, products.reshape(FRAMES, -1), precision=highest)
    binned = binned.reshape(BINS, 2, OUTCH, STATIONS, STATIONS)

    def pick(block):
        row_start = (block // NGRP * GROUP_ST).astype(jnp.int32)
        col_start = (block % NGRP * GROUP_ST).astype(jnp.int32)
        row_band = lax.dynamic_slice_in_dim(binned, row_start, GROUP_ST, 3)
        block_tile = lax.dynamic_slice_in_dim(row_band, col_start, GROUP_ST, 4)
        return block_tile.transpose(0, 1, 3, 4, 2).reshape(BINS, 2, GROUP_ST * GROUP_ST, OUTCH)
    return jax.vmap(pick, out_axes=1)(assignment)
```

```python
import functools
import math

import jax
import jax.numpy as jnp
import numpy as np
from jax import lax
from jax.experimental import pallas as pl
from jax.experimental.pallas import tpu as pltpu
from jax.sharding import PartitionSpec as P

NCHAN = 8192
GROUP_ST = 8
RADIX_A = 16
CHAVG = 64
NGRP = 4
OUTCH = 128
BINS = 32
DELAY_MAX = 49152
LANES = 128
RADIX_B = NCHAN // RADIX_A
QUADS = RADIX_B // LANES
F32, BF16 = jnp.float32, jnp.bfloat16
AXES = ("tm", "pair")


def section_tables(stations):
    a, b = np.arange(RADIX_A), np.arange(RADIX_B)
    angle = ((a[:, None] * a[None, :]) % RADIX_A).astype(np.float32) * np.float32(2.0 * math.pi / RADIX_A)
    cos_a = (np.cos(angle) * np.float32(1.0 / math.sqrt(RADIX_A))).astype(np.float32)
    sin_a = (np.sin(angle) * np.float32(1.0 / math.sqrt(RADIX_A))).astype(np.float32)
    small = np.stack([np.stack([cos_a, sin_a], 1), np.stack([-sin_a, cos_a], 1)], 0)
    first = np.einsum("st,pkrn->psktrn", np.eye(stations, dtype=np.float32), small)
    rows = 2 * stations * RADIX_A
    first = first.reshape(rows, rows)
    turn = (a[:, None] * b[None, :]).astype(np.float32) * np.float32(2.0 * math.pi / NCHAN)
    twist = np.stack([np.cos(turn), np.sin(turn)]).astype(np.float32)
    twist = np.tile(twist, (1, stations, 1))
    angle = ((b[:, None] * b[None, :]) % RADIX_B).astype(np.float32) * np.float32(2.0 * math.pi / RADIX_B)
    cos_b = (np.cos(angle) * np.float32(1.0 / math.sqrt(RADIX_B))).astype(np.float32)
    sin_b = (np.sin(angle) * np.float32(1.0 / math.sqrt(RADIX_B))).astype(np.float32)
    second = np.stack([np.stack([cos_b, -sin_b], 1), np.stack([sin_b, cos_b], 1)], 0)
    second = second.reshape(2, RADIX_B, 2, OUTCH, QUADS).transpose(0, 1, 4, 2, 3)
    second = second.reshape(2 * RADIX_B, 2 * RADIX_B)
    return jnp.asarray(first, BF16), jnp.asarray(twist), jnp.asarray(second, BF16)


def spectra_kernel(dims, delays, own, following, beyond, first, twist, second, phase, out,
                   series, windows, turned, planes, rows):
    frames, stations = dims
    held, ahead, last = own.shape[2], following.shape[2], beyond.shape[2]
    sk = stations * RADIX_A

    def widen(s, carry):
        for r in range(2):
            series[r, s, 0:held] = own[r, s].astype(F32)
            series[r, s, held:held + ahead] = following[r, s].astype(F32)
            series[r, s, held + ahead:held + ahead + last] = beyond[r, s].astype(F32)
            series[r, s, held + ahead + last:] = jnp.zeros((8, LANES), F32)
        return carry

    lax.fori_loop(0, stations, widen, 0)
    lane = lax.broadcasted_iota(jnp.int32, (RADIX_A, LANES), 1)

    def one_frame(f, carry):
        for s in range(stations):
            offset = f * NCHAN + delays[s, f]
            row, shift = offset // LANES, offset % LANES
            for r in range(2):
                parts = [
                    pltpu.roll(series[r, s, pl.ds(row + h, RADIX_A, stride=QUADS), :], (LANES - shift) % LANES, 1)
                    for h in range(QUADS + 1)
                ]
                for h in range(QUADS):
                    cut = jnp.where(lane < LANES - shift, parts[h], parts[h + 1])
                    windows[(2 * s + r) * RADIX_A:(2 * s + r + 1) * RADIX_A, h * LANES:(h + 1) * LANES] = cut.astype(BF16)
        passed = jnp.dot(first[...], windows[...], preferred_element_type=F32)
        real, imag = passed[:sk], passed[sk:]
        here = pl.ds(pl.multiple_of(f * sk, sk), sk)
        turned[here, 0:RADIX_B] = (real * twist[0] + imag * twist[1]).astype(BF16)
        turned[here, RADIX_B:] = (imag * twist[0] - real * twist[1]).astype(BF16)
        return carry

    lax.fori_loop(0, frames, one_frame, 0)
    for g in range(QUADS):
        channels = jnp.dot(turned[...], second[:, g * 2 * LANES:(g + 1) * 2 * LANES], preferred_element_type=F32)
        real = channels[:, :LANES].reshape(frames, sk, LANES)
        imag = channels[:, LANES:].reshape(frames, sk, LANES)
        cosine, sine = phase[0, g], phase[1, g]
        turned_re = (real * cosine - imag * sine).reshape(frames * stations, RADIX_A, LANES)
        turned_im = (real * sine + imag * cosine).reshape(frames * stations, RADIX_A, LANES)
        planes[:, g * RADIX_A:(g + 1) * RADIX_A, :] = turned_re
        planes[:, CHAVG + g * RADIX_A:CHAVG + (g + 1) * RADIX_A, :] = turned_im

    count = frames * stations

    def flip(i, carry):
        rows[pl.ds(i, OUTCH, stride=count), :] = planes[i].T
        return carry

    lax.fori_loop(0, count, flip, 0, unroll=4)
    out[...] = rows[...].astype(BF16).reshape(out.shape)


def product_kernel(dims, bins, assignment, spectra, out, sums):
    owners, pairs, group, slots = dims
    depth, frames = spectra.shape[2], spectra.shape[3]
    pairings = depth // group
    stations = pairs * spectra.shape[4]
    sums[...] = jnp.zeros_like(sums)
    lane = lax.broadcasted_iota(jnp.int32, (stations, LANES), 1)

    def one_owner(t, carry):
        for f in range(frames):
            b = bins[t * frames + f]
            for op in range(pairings):
                grams = []
                for o2 in range(group):
                    held = [spectra[t, p, op * group + o2, f].astype(F32) for p in range(pairs)]
                    left = jnp.concatenate(held, 0)
                    swapped = pltpu.roll(left, CHAVG, 1)
                    swapped = jnp.where(lane < CHAVG, -swapped, swapped)
                    right = jnp.concatenate([left, swapped], 0).astype(BF16)
                    grams.append(lax.dot_general(
                        left.astype(BF16), right, (((1,), (1,)), ((), ())), preferred_element_type=F32))
                if group == 1:
                    grams.append(jnp.zeros_like(grams[0]))
                sums[b, op] += jnp.concatenate(grams, 1)
        return carry

    lax.fori_loop(0, owners, one_owner, 0)
    width = slots * 2 * GROUP_ST
    source = lax.broadcasted_iota(jnp.int32, (LANES, LANES), 0)
    target = lax.broadcasted_iota(jnp.int32, (LANES, LANES), 1)
    slot_of = (target // (2 * GROUP_ST)) % slots
    wanted = (target // width) * (2 * stations) + (target // GROUP_ST) % 2 * stations + target % GROUP_ST
    inside = target < group * width
    total = sums.shape[0] * pairings * GROUP_ST
    for p in range(pairs):
        moved = jnp.zeros((total, LANES), F32)
        for k in range(slots):
            block = assignment[p * slots + k]
            top = pl.multiple_of(block // NGRP * GROUP_ST, GROUP_ST)
            left = block % NGRP * GROUP_ST
            lines = sums[:, :, pl.ds(top, GROUP_ST), :].reshape(total, LANES)
            pick = (source == wanted + left) & (slot_of == k) & inside
            moved += jnp.dot(
                (lines * (1.0 / CHAVG)).astype(BF16),
                jnp.where(pick, 1.0, 0.0).astype(BF16),
                preferred_element_type=F32)
        out[:, p] = moved.reshape(owners, -1, pairings * GROUP_ST, LANES).astype(BF16)


def place_kernel(dims, received, out, lines):
    replicas, depth, group = dims
    count, here, rows_of = received.shape[0], received.shape[1], received.shape[2]
    pairings = rows_of // GROUP_ST
    slots = out.shape[1]
    width = slots * 2 * GROUP_ST
    lines[...] = received[...].reshape(lines.shape).astype(F32)
    row = lax.broadcasted_iota(jnp.int32, (pairings * count, OUTCH), 0)
    lane = lax.broadcasted_iota(jnp.int32, (pairings * count, OUTCH), 1)
    device, op = row % count, row // count
    places = []
    for o2 in range(group):
        channel = device // replicas * depth + op * group + o2
        hit = (channel == lane) & (device % replicas == 0)
        places.append(jnp.where(hit, 1.0, 0.0).astype(BF16))

    def one(step, carry):
        b, p = step // GROUP_ST, step % GROUP_ST
        sent = [
            lines[pl.ds(b * rows_of + op * GROUP_ST + p, count, stride=here * rows_of), :]
            for op in range(pairings)
        ]
        sent = jnp.concatenate(sent, 0)
        value = jnp.zeros((width, OUTCH), F32)
        for o2 in range(group):
            part = sent[:, o2 * width:(o2 + 1) * width].astype(BF16)
            value += lax.dot_general(
                part, places[o2], (((0,), (0,)), ((), ())), preferred_element_type=F32)
        value = value.reshape(slots, 2, GROUP_ST, OUTCH)
        out[b, :, :, pl.ds(pl.multiple_of(p * GROUP_ST, GROUP_ST), GROUP_ST), :] = value
        return carry

    lax.fori_loop(0, here * GROUP_ST, one, 0, unroll=2)


VMEM = pl.BlockSpec(memory_space=pltpu.VMEM)
SMEM = pl.BlockSpec(memory_space=pltpu.SMEM)
PARAMS = pltpu.CompilerParams(vmem_limit_bytes=48 * 1024 * 1024)


def from_behind(value, axis, steps):
    count = lax.axis_size(axis)
    first, last = (max(0, -steps), min(count, count - steps))
    return lax.ppermute(value, axis, [(source, source + steps) for source in range(first, last)])


def exchange(value):
    return lax.all_to_all(value, AXES, split_axis=0, concat_axis=0, tiled=True)


def body(voltages, delays, phase_model, phase_bins, assignment):
    owners, pairs = lax.axis_size("tm"), lax.axis_size("pair")
    devices = owners * pairs
    stations, samples = voltages.shape[1], voltages.shape[2]
    frames = samples // NCHAN
    slots = assignment.shape[0]
    channel_groups = min(devices, OUTCH)
    depth = OUTCH // channel_groups
    replicas = devices // channel_groups
    group = min(2, depth)
    count = frames * stations

    first, twist, second = section_tables(stations)
    lines = voltages.reshape(2, stations, samples // LANES, LANES)
    ahead = min(DELAY_MAX, samples)
    last = DELAY_MAX - ahead
    following = from_behind(lines[:, :, :ahead // LANES], "tm", -1)
    beyond = from_behind(lines[:, :, :last // LANES], "tm", -2)

    every_bin = lax.all_gather(phase_bins, "tm", axis=0, tiled=True)
    every_slot = lax.all_gather(assignment, "pair", axis=0, tiled=True)

    angles = lax.dynamic_slice_in_dim(phase_model, lax.axis_index("pair") * stations, stations, 0)
    angles = angles.reshape(stations, OUTCH, QUADS, RADIX_A).transpose(2, 0, 3, 1)
    angles = angles.reshape(QUADS, stations * RADIX_A, OUTCH)
    phase = jnp.stack([jnp.cos(angles), jnp.sin(angles)])

    total_rows = (samples + DELAY_MAX) // LANES + 8
    sk = stations * RADIX_A
    spectra = pl.pallas_call(
        functools.partial(spectra_kernel, (frames, stations)),
        out_shape=jax.ShapeDtypeStruct((OUTCH, count, LANES), BF16),
        in_specs=[SMEM] + [VMEM] * 7,
        out_specs=VMEM,
        scratch_shapes=[
            pltpu.VMEM((2, stations, total_rows, LANES), F32),
            pltpu.VMEM((2 * sk, RADIX_B), BF16),
            pltpu.VMEM((frames * sk, 2 * RADIX_B), BF16),
            pltpu.VMEM((count, LANES, LANES), F32),
            pltpu.VMEM((OUTCH * count, LANES), F32),
        ],
        compiler_params=PARAMS,
        name="spectra",
    )(delays, lines, following, beyond, first, twist, second, phase)

    sent = spectra.reshape(channel_groups, depth * count, LANES)
    if replicas > 1:
        sent = jnp.repeat(sent, replicas, axis=0)
    routed = exchange(sent)
    routed = routed.reshape(owners, pairs, depth, frames, stations, LANES)

    all_bins = BINS
    bins_here = all_bins // owners
    rows_of = depth // group * GROUP_ST
    binned = pl.pallas_call(
        functools.partial(product_kernel, (owners, pairs, group, slots)),
        out_shape=jax.ShapeDtypeStruct((owners, pairs, bins_here, rows_of, LANES), BF16),
        in_specs=[SMEM, SMEM, VMEM],
        out_specs=VMEM,
        scratch_shapes=[pltpu.VMEM((all_bins, depth // group, pairs * stations, LANES), F32)],
        compiler_params=PARAMS,
        name="products",
    )(every_bin, every_slot, routed)

    returned = exchange(binned.reshape(devices, bins_here, rows_of, LANES))
    return pl.pallas_call(
        functools.partial(place_kernel, (replicas, depth, group)),
        out_shape=jax.ShapeDtypeStruct((bins_here, slots, 2, GROUP_ST * GROUP_ST, OUTCH), F32),
        in_specs=[VMEM],
        out_specs=VMEM,
        scratch_shapes=[pltpu.VMEM((devices * bins_here * rows_of, LANES), F32)],
        compiler_params=PARAMS,
        name="place",
    )(returned)


def solution(mesh):
    in_specs = (P(None, "pair", "tm"), P("pair", "tm"), P(), P("tm"), P("pair"))
    out_specs = P("tm", "pair", None, None, None)
    return jax.shard_map(body, mesh=mesh, in_specs=in_specs, out_specs=out_specs, check_vma=False)
```

```python
import functools
import math

import jax
import jax.numpy as jnp
import numpy as np
from jax import lax
from jax.experimental import pallas as pl
from jax.experimental.pallas import tpu as pltpu
from jax.sharding import PartitionSpec as P

NCHAN = 8192
GROUP_ST = 8
RADIX_A = 16
CHAVG = 64
NGRP = 4
OUTCH = 128
BINS = 32
DELAY_MAX = 49152
LANES = 128
RADIX_B = NCHAN // RADIX_A
QUADS = RADIX_B // LANES
F32, BF16 = jnp.float32, jnp.bfloat16
AXES = ("tm", "pair")


def section_tables(stations):
    a, b = np.arange(RADIX_A), np.arange(RADIX_B)
    angle = ((a[:, None] * a[None, :]) % RADIX_A).astype(np.float32) * np.float32(2.0 * math.pi / RADIX_A)
    cos_a = (np.cos(angle) * np.float32(1.0 / math.sqrt(RADIX_A))).astype(np.float32)
    sin_a = (np.sin(angle) * np.float32(1.0 / math.sqrt(RADIX_A))).astype(np.float32)
    small = np.stack([np.stack([cos_a, sin_a], 1), np.stack([-sin_a, cos_a], 1)], 0)
    first = np.einsum("st,pkrn->psktrn", np.eye(stations, dtype=np.float32), small)
    rows = 2 * stations * RADIX_A
    first = first.reshape(rows, rows)
    turn = (a[:, None] * b[None, :]).astype(np.float32) * np.float32(2.0 * math.pi / NCHAN)
    twist = np.stack([np.cos(turn), np.sin(turn)]).astype(np.float32)
    twist = np.tile(twist, (1, stations, 1))
    angle = ((b[:, None] * b[None, :]) % RADIX_B).astype(np.float32) * np.float32(2.0 * math.pi / RADIX_B)
    cos_b = (np.cos(angle) * np.float32(1.0 / math.sqrt(RADIX_B))).astype(np.float32)
    sin_b = (np.sin(angle) * np.float32(1.0 / math.sqrt(RADIX_B))).astype(np.float32)
    second = np.stack([np.stack([cos_b, -sin_b], 1), np.stack([sin_b, cos_b], 1)], 0)
    second = second.reshape(2, RADIX_B, 2, OUTCH, QUADS).transpose(0, 1, 4, 2, 3)
    second = second.reshape(2 * RADIX_B, 2 * RADIX_B)
    return jnp.asarray(first, BF16), jnp.asarray(twist), jnp.asarray(second, BF16)


def spectra_kernel(dims, delays, ahead_of, own, following, beyond, first, twist, second, phase, out,
                   series, windows, turned, planes, rows):
    frames, stations = dims
    held, ahead, last = own.shape[2], following.shape[2], beyond.shape[2]
    sk = stations * RADIX_A

    def widen(s, carry):
        for r in range(2):
            series[r, s, 0:held] = own[r, s].astype(F32)
            series[r, s, held:held + ahead] = following[r, s].astype(F32)
            series[r, s, held + ahead:held + ahead + last] = beyond[r, s].astype(F32)
            series[r, s, held + ahead + last:] = jnp.zeros((8, LANES), F32)
        return carry

    lax.fori_loop(0, stations, widen, 0)
    lane = lax.broadcasted_iota(jnp.int32, (RADIX_A, LANES), 1)

    def one_frame(f, carry):
        for s in range(stations):
            offset = f * NCHAN + delays[s, f]
            row, shift = offset // LANES, offset % LANES
            for r in range(2):
                parts = [
                    pltpu.roll(series[r, s, pl.ds(row + h, RADIX_A, stride=QUADS), :], (LANES - shift) % LANES, 1)
                    for h in range(QUADS + 1)
                ]
                for h in range(QUADS):
                    cut = jnp.where(lane < LANES - shift, parts[h], parts[h + 1])
                    windows[(2 * s + r) * RADIX_A:(2 * s + r + 1) * RADIX_A, h * LANES:(h + 1) * LANES] = cut.astype(BF16)
        passed = jnp.dot(first[...], windows[...], preferred_element_type=F32)
        real, imag = passed[:sk], passed[sk:]
        here = pl.ds(pl.multiple_of(f * sk, sk), sk)
        turned[here, 0:RADIX_B] = (real * twist[0] + imag * twist[1]).astype(BF16)
        turned[here, RADIX_B:] = (imag * twist[0] - real * twist[1]).astype(BF16)
        return carry

    lax.fori_loop(0, frames, one_frame, 0)
    for g in range(QUADS):
        channels = jnp.dot(turned[...], second[:, g * 2 * LANES:(g + 1) * 2 * LANES], preferred_element_type=F32)
        real = channels[:, :LANES].reshape(frames, sk, LANES)
        imag = channels[:, LANES:].reshape(frames, sk, LANES)
        cosine, sine = phase[0, g], phase[1, g]
        turned_re = (real * cosine - imag * sine).reshape(frames * stations, RADIX_A, LANES)
        turned_im = (real * sine + imag * cosine).reshape(frames * stations, RADIX_A, LANES)
        planes[:, g * RADIX_A:(g + 1) * RADIX_A, :] = turned_re
        planes[:, CHAVG + g * RADIX_A:CHAVG + (g + 1) * RADIX_A, :] = turned_im

    count = frames * stations

    def flip(i, carry):
        rows[pl.ds(i, OUTCH, stride=count), :] = planes[i].T
        return carry

    lax.fori_loop(0, count, flip, 0, unroll=4)
    out[...] = rows[...].astype(BF16).reshape(out.shape)


def product_kernel(dims, bins, assignment, spectra, out, sums):
    owners, pairs, group, slots = dims
    depth, frames = spectra.shape[2], spectra.shape[3]
    pairings = depth // group
    stations = pairs * spectra.shape[4]
    sums[...] = jnp.zeros_like(sums)
    lane = lax.broadcasted_iota(jnp.int32, (stations, LANES), 1)

    def one_owner(t, carry):
        for f in range(frames):
            b = bins[t * frames + f]
            for op in range(pairings):
                grams = []
                for o2 in range(group):
                    held = [spectra[t, p, op * group + o2, f].astype(F32) for p in range(pairs)]
                    left = jnp.concatenate(held, 0)
                    swapped = pltpu.roll(left, CHAVG, 1)
                    swapped = jnp.where(lane < CHAVG, -swapped, swapped)
                    right = jnp.concatenate([left, swapped], 0).astype(BF16)
                    grams.append(lax.dot_general(
                        left.astype(BF16), right, (((1,), (1,)), ((), ())), preferred_element_type=F32))
                if group == 1:
                    grams.append(jnp.zeros_like(grams[0]))
                sums[b, op] += jnp.concatenate(grams, 1)
        return carry

    lax.fori_loop(0, owners, one_owner, 0)
    width = slots * 2 * GROUP_ST
    source = lax.broadcasted_iota(jnp.int32, (LANES, LANES), 0)
    target = lax.broadcasted_iota(jnp.int32, (LANES, LANES), 1)
    slot_of = (target // (2 * GROUP_ST)) % slots
    wanted = (target // width) * (2 * stations) + (target // GROUP_ST) % 2 * stations + target % GROUP_ST
    inside = target < group * width
    total = sums.shape[0] * pairings * GROUP_ST
    for p in range(pairs):
        moved = jnp.zeros((total, LANES), F32)
        for k in range(slots):
            block = assignment[p * slots + k]
            top = pl.multiple_of(block // NGRP * GROUP_ST, GROUP_ST)
            left = block % NGRP * GROUP_ST
            lines = sums[:, :, pl.ds(top, GROUP_ST), :].reshape(total, LANES)
            pick = (source == wanted + left) & (slot_of == k) & inside
            moved += jnp.dot(
                (lines * (1.0 / CHAVG)).astype(BF16),
                jnp.where(pick, 1.0, 0.0).astype(BF16),
                preferred_element_type=F32)
        out[:, p] = moved.reshape(owners, -1, pairings * GROUP_ST, LANES).astype(BF16)


def place_kernel(dims, received, out, lines):
    replicas, depth, group = dims
    count, here, rows_of = received.shape[0], received.shape[1], received.shape[2]
    pairings = rows_of // GROUP_ST
    slots = out.shape[1]
    width = slots * 2 * GROUP_ST
    lines[...] = received[...].reshape(lines.shape).astype(F32)
    row = lax.broadcasted_iota(jnp.int32, (pairings * count, OUTCH), 0)
    lane = lax.broadcasted_iota(jnp.int32, (pairings * count, OUTCH), 1)
    device, op = row % count, row // count
    places = []
    for o2 in range(group):
        channel = device // replicas * depth + op * group + o2
        hit = (channel == lane) & (device % replicas == 0)
        places.append(jnp.where(hit, 1.0, 0.0).astype(BF16))

    def one(step, carry):
        b, p = step // GROUP_ST, step % GROUP_ST
        sent = [
            lines[pl.ds(b * rows_of + op * GROUP_ST + p, count, stride=here * rows_of), :]
            for op in range(pairings)
        ]
        sent = jnp.concatenate(sent, 0)
        value = jnp.zeros((width, OUTCH), F32)
        for o2 in range(group):
            part = sent[:, o2 * width:(o2 + 1) * width].astype(BF16)
            value += lax.dot_general(
                part, places[o2], (((0,), (0,)), ((), ())), preferred_element_type=F32)
        value = value.reshape(slots, 2, GROUP_ST, OUTCH)
        out[b, :, :, pl.ds(pl.multiple_of(p * GROUP_ST, GROUP_ST), GROUP_ST), :] = value
        return carry

    lax.fori_loop(0, here * GROUP_ST, one, 0, unroll=8)


VMEM = pl.BlockSpec(memory_space=pltpu.VMEM)
SMEM = pl.BlockSpec(memory_space=pltpu.SMEM)
PARAMS = pltpu.CompilerParams(vmem_limit_bytes=48 * 1024 * 1024)


def from_behind(value, axis, steps):
    count = lax.axis_size(axis)
    first, last = (max(0, -steps), min(count, count - steps))
    return lax.ppermute(value, axis, [(source, source + steps) for source in range(first, last)])


def exchange_kernel(dims, sent, received, send_sems, recv_sems, own_sem):
    owners, pairs = dims
    devices = owners * pairs
    me = lax.axis_index("tm") * pairs + lax.axis_index("pair")
    barrier = pltpu.get_barrier_semaphore()

    def place_of(device):
        return (device // pairs, device % pairs)

    def greet(step, carry):
        peer = (me + step) % devices
        pl.semaphore_signal(barrier, inc=1, device_id=place_of(peer), device_id_type=pl.DeviceIdType.MESH)
        return carry

    lax.fori_loop(1, devices, greet, 0)
    pl.semaphore_wait(barrier, devices - 1)

    def copy_to(step):
        peer = (me + step) % devices
        return pltpu.make_async_remote_copy(
            src_ref=sent.at[peer], dst_ref=received.at[me],
            send_sem=send_sems.at[step], recv_sem=recv_sems.at[step],
            device_id=place_of(peer), device_id_type=pl.DeviceIdType.MESH)

    def copy_from(step):
        peer = (me + devices - step) % devices
        return pltpu.make_async_remote_copy(
            src_ref=sent.at[peer], dst_ref=received.at[peer],
            send_sem=send_sems.at[step], recv_sem=recv_sems.at[step],
            device_id=place_of(peer), device_id_type=pl.DeviceIdType.MESH)

    def start(step, carry):
        copy_to(step).start()
        return carry

    lax.fori_loop(1, devices, start, 0)
    own = pltpu.make_async_copy(sent.at[me], received.at[me], own_sem)
    own.start()
    own.wait()

    def finish(step, carry):
        copy_to(step).wait_send()
        copy_from(step).wait_recv()
        return carry

    lax.fori_loop(1, devices, finish, 0)


def exchange(value, number):
    owners, pairs = lax.axis_size("tm"), lax.axis_size("pair")
    devices = owners * pairs
    return pl.pallas_call(
        functools.partial(exchange_kernel, (owners, pairs)),
        out_shape=jax.ShapeDtypeStruct(value.shape, value.dtype),
        in_specs=[VMEM],
        out_specs=VMEM,
        scratch_shapes=[
            pltpu.SemaphoreType.DMA((devices,)),
            pltpu.SemaphoreType.DMA((devices,)),
            pltpu.SemaphoreType.DMA,
        ],
        compiler_params=pltpu.CompilerParams(collective_id=number, has_side_effects=True),
        name="exchange",
    )(value)


def body(voltages, delays, phase_model, phase_bins, assignment):
    owners, pairs = lax.axis_size("tm"), lax.axis_size("pair")
    devices = owners * pairs
    stations, samples = voltages.shape[1], voltages.shape[2]
    frames = samples // NCHAN
    slots = assignment.shape[0]
    channel_groups = min(devices, OUTCH)
    depth = OUTCH // channel_groups
    replicas = devices // channel_groups
    group = min(2, depth)
    count = frames * stations

    first, twist, second = section_tables(stations)
    lines = voltages.reshape(2, stations, samples // LANES, LANES)
    ahead = min(DELAY_MAX, samples)
    last = DELAY_MAX - ahead
    following = from_behind(lines[:, :, :ahead // LANES], "tm", -1)
    beyond = from_behind(lines[:, :, :last // LANES], "tm", -2)

    small = lax.all_gather(jnp.concatenate([phase_bins, assignment]), AXES, axis=0)
    small = small.reshape(owners, pairs, -1)
    every_bin = small[:, 0, :frames].reshape(-1)
    every_slot = small[0, :, frames:].reshape(-1)

    angles = lax.dynamic_slice_in_dim(phase_model, lax.axis_index("pair") * stations, stations, 0)
    angles = angles.reshape(stations, OUTCH, QUADS, RADIX_A).transpose(2, 0, 3, 1)
    angles = angles.reshape(QUADS, stations * RADIX_A, OUTCH)
    phase = jnp.stack([jnp.cos(angles), jnp.sin(angles)])

    total_rows = (samples + DELAY_MAX) // LANES + 8
    sk = stations * RADIX_A
    spectra = pl.pallas_call(
        functools.partial(spectra_kernel, (frames, stations)),
        out_shape=jax.ShapeDtypeStruct((OUTCH, count, LANES), BF16),
        in_specs=[SMEM, SMEM] + [VMEM] * 7,
        out_specs=VMEM,
        scratch_shapes=[
            pltpu.VMEM((2, stations, total_rows, LANES), F32),
            pltpu.VMEM((2 * sk, RADIX_B), BF16),
            pltpu.VMEM((frames * sk, 2 * RADIX_B), BF16),
            pltpu.VMEM((count, LANES, LANES), F32),
            pltpu.VMEM((OUTCH * count, LANES), F32),
        ],
        compiler_params=PARAMS,
        name="spectra",
    )(delays, every_bin, lines, following, beyond, first, twist, second, phase)

    sent = spectra.reshape(channel_groups, depth * count, LANES)
    if replicas > 1:
        sent = jnp.repeat(sent, replicas, axis=0)
    routed = exchange(sent, 0)
    routed = routed.reshape(owners, pairs, depth, frames, stations, LANES)

    all_bins = BINS
    bins_here = all_bins // owners
    rows_of = depth // group * GROUP_ST
    binned = pl.pallas_call(
        functools.partial(product_kernel, (owners, pairs, group, slots)),
        out_shape=jax.ShapeDtypeStruct((owners, pairs, bins_here, rows_of, LANES), BF16),
        in_specs=[SMEM, SMEM, VMEM],
        out_specs=VMEM,
        scratch_shapes=[pltpu.VMEM((all_bins, depth // group, pairs * stations, LANES), F32)],
        compiler_params=PARAMS,
        name="products",
    )(every_bin, every_slot, routed)

    returned = exchange(binned.reshape(devices, bins_here, rows_of, LANES), 1)
    return pl.pallas_call(
        functools.partial(place_kernel, (replicas, depth, group)),
        out_shape=jax.ShapeDtypeStruct((bins_here, slots, 2, GROUP_ST * GROUP_ST, OUTCH), F32),
        in_specs=[VMEM],
        out_specs=VMEM,
        scratch_shapes=[pltpu.VMEM((devices * bins_here * rows_of, LANES), F32)],
        compiler_params=PARAMS,
        name="place",
    )(returned)


def solution(mesh):
    in_specs = (P(None, "pair", "tm"), P("pair", "tm"), P(), P("tm"), P("pair"))
    out_specs = P("tm", "pair", None, None, None)
    return jax.shard_map(body, mesh=mesh, in_specs=in_specs, out_specs=out_specs, check_vma=False)
```

```python
import functools
import math

import jax
import jax.numpy as jnp
import numpy as np
from jax import lax
from jax.experimental import pallas as pl
from jax.experimental.pallas import tpu as pltpu
from jax.sharding import PartitionSpec as P

NCHAN = 8192
GROUP_ST = 8
RADIX_A = 16
CHAVG = 64
NGRP = 4
OUTCH = 128
BINS = 32
DELAY_MAX = 49152
LANES = 128
RADIX_B = NCHAN // RADIX_A
QUADS = RADIX_B // LANES
F32, BF16 = jnp.float32, jnp.bfloat16
AXES = ("tm", "pair")


def section_tables(stations):
    a, b = np.arange(RADIX_A), np.arange(RADIX_B)
    angle = ((a[:, None] * a[None, :]) % RADIX_A).astype(np.float32) * np.float32(2.0 * math.pi / RADIX_A)
    cos_a = (np.cos(angle) * np.float32(1.0 / math.sqrt(RADIX_A))).astype(np.float32)
    sin_a = (np.sin(angle) * np.float32(1.0 / math.sqrt(RADIX_A))).astype(np.float32)
    small = np.stack([np.stack([cos_a, sin_a], 1), np.stack([-sin_a, cos_a], 1)], 0)
    first = np.einsum("st,pkrn->psktrn", np.eye(stations, dtype=np.float32), small)
    rows = 2 * stations * RADIX_A
    first = first.reshape(rows, rows)
    turn = (a[:, None] * b[None, :]).astype(np.float32) * np.float32(2.0 * math.pi / NCHAN)
    twist = np.stack([np.cos(turn), np.sin(turn)]).astype(np.float32)
    twist = np.tile(twist, (1, stations, 1))
    angle = ((b[:, None] * b[None, :]) % RADIX_B).astype(np.float32) * np.float32(2.0 * math.pi / RADIX_B)
    cos_b = (np.cos(angle) * np.float32(1.0 / math.sqrt(RADIX_B))).astype(np.float32)
    sin_b = (np.sin(angle) * np.float32(1.0 / math.sqrt(RADIX_B))).astype(np.float32)
    second = np.stack([np.stack([cos_b, -sin_b], 1), np.stack([sin_b, cos_b], 1)], 0)
    second = second.reshape(2, RADIX_B, 2, OUTCH, QUADS).transpose(0, 1, 4, 2, 3)
    second = second.reshape(2 * RADIX_B, 2 * RADIX_B)
    return jnp.asarray(first, BF16), jnp.asarray(twist), jnp.asarray(second, BF16)


def spectra_kernel(dims, delays, own, following, beyond, first, twist, second, phase, out,
                   series, windows, turned, planes, rows):
    frames, stations = dims
    held, ahead, last = own.shape[2], following.shape[2], beyond.shape[2]
    sk = stations * RADIX_A

    def widen(s, carry):
        for r in range(2):
            series[r, s, 0:held] = own[r, s].astype(F32)
            series[r, s, held:held + ahead] = following[r, s].astype(F32)
            series[r, s, held + ahead:held + ahead + last] = beyond[r, s].astype(F32)
            series[r, s, held + ahead + last:] = jnp.zeros((8, LANES), F32)
        return carry

    lax.fori_loop(0, stations, widen, 0)
    lane = lax.broadcasted_iota(jnp.int32, (RADIX_A, LANES), 1)

    def one_frame(f, carry):
        for s in range(stations):
            offset = f * NCHAN + delays[s, f]
            row, shift = offset // LANES, offset % LANES
            for r in range(2):
                parts = [
                    pltpu.roll(series[r, s, pl.ds(row + h, RADIX_A, stride=QUADS), :], (LANES - shift) % LANES, 1)
                    for h in range(QUADS + 1)
                ]
                for h in range(QUADS):
                    cut = jnp.where(lane < LANES - shift, parts[h], parts[h + 1])
                    windows[(2 * s + r) * RADIX_A:(2 * s + r + 1) * RADIX_A, h * LANES:(h + 1) * LANES] = cut.astype(BF16)
        passed = jnp.dot(first[...], windows[...], preferred_element_type=F32)
        real, imag = passed[:sk], passed[sk:]
        here = pl.ds(pl.multiple_of(f * sk, sk), sk)
        turned[here, 0:RADIX_B] = (real * twist[0] + imag * twist[1]).astype(BF16)
        turned[here, RADIX_B:] = (imag * twist[0] - real * twist[1]).astype(BF16)
        return carry

    lax.fori_loop(0, frames, one_frame, 0)
    for g in range(QUADS):
        channels = jnp.dot(turned[...], second[:, g * 2 * LANES:(g + 1) * 2 * LANES], preferred_element_type=F32)
        real = channels[:, :LANES].reshape(frames, sk, LANES)
        imag = channels[:, LANES:].reshape(frames, sk, LANES)
        cosine, sine = phase[0, g], phase[1, g]
        turned_re = (real * cosine - imag * sine).reshape(frames * stations, RADIX_A, LANES)
        turned_im = (real * sine + imag * cosine).reshape(frames * stations, RADIX_A, LANES)
        planes[:, g * RADIX_A:(g + 1) * RADIX_A, :] = turned_re
        planes[:, CHAVG + g * RADIX_A:CHAVG + (g + 1) * RADIX_A, :] = turned_im

    count = frames * stations

    def flip(i, carry):
        rows[pl.ds(i, OUTCH, stride=count), :] = planes[i].T
        return carry

    lax.fori_loop(0, count, flip, 0, unroll=4)
    out[...] = rows[...].astype(BF16).reshape(out.shape)


def product_kernel(dims, small, spectra, out, sums):
    owners, pairs, group, slots = dims
    depth, frames = spectra.shape[2], spectra.shape[3]
    pairings = depth // group
    stations = pairs * spectra.shape[4]
    sums[...] = jnp.zeros_like(sums)
    lane = lax.broadcasted_iota(jnp.int32, (stations, LANES), 1)

    def one_owner(t, carry):
        for f in range(frames):
            b = small[t * pairs, f]
            for op in range(pairings):
                grams = []
                for o2 in range(group):
                    held = [spectra[t, p, op * group + o2, f].astype(F32) for p in range(pairs)]
                    left = jnp.concatenate(held, 0)
                    swapped = pltpu.roll(left, CHAVG, 1)
                    swapped = jnp.where(lane < CHAVG, -swapped, swapped)
                    right = jnp.concatenate([left, swapped], 0).astype(BF16)
                    grams.append(lax.dot_general(
                        left.astype(BF16), right, (((1,), (1,)), ((), ())), preferred_element_type=F32))
                if group == 1:
                    grams.append(jnp.zeros_like(grams[0]))
                sums[b, op] += jnp.concatenate(grams, 1)
        return carry

    lax.fori_loop(0, owners, one_owner, 0)
    width = slots * 2 * GROUP_ST
    source = lax.broadcasted_iota(jnp.int32, (LANES, LANES), 0)
    target = lax.broadcasted_iota(jnp.int32, (LANES, LANES), 1)
    slot_of = (target // (2 * GROUP_ST)) % slots
    wanted = (target // width) * (2 * stations) + (target // GROUP_ST) % 2 * stations + target % GROUP_ST
    inside = target < group * width
    total = sums.shape[0] * pairings * GROUP_ST
    for p in range(pairs):
        moved = jnp.zeros((total, LANES), F32)
        for k in range(slots):
            block = small[p, frames + k]
            top = pl.multiple_of(block // NGRP * GROUP_ST, GROUP_ST)
            left = block % NGRP * GROUP_ST
            lines = sums[:, :, pl.ds(top, GROUP_ST), :].reshape(total, LANES)
            pick = (source == wanted + left) & (slot_of == k) & inside
            moved += jnp.dot(
                (lines * (1.0 / CHAVG)).astype(BF16),
                jnp.where(pick, 1.0, 0.0).astype(BF16),
                preferred_element_type=F32)
        out[:, p] = moved.reshape(owners, -1, pairings * GROUP_ST, LANES).astype(BF16)


def place_kernel(dims, received, out, lines):
    replicas, depth, group = dims
    count, here, rows_of = received.shape[0], received.shape[1], received.shape[2]
    pairings = rows_of // GROUP_ST
    slots = out.shape[1]
    width = slots * 2 * GROUP_ST
    lines[...] = received[...].reshape(lines.shape).astype(F32)
    row = lax.broadcasted_iota(jnp.int32, (pairings * count, OUTCH), 0)
    lane = lax.broadcasted_iota(jnp.int32, (pairings * count, OUTCH), 1)
    device, op = row % count, row // count
    places = []
    for o2 in range(group):
        channel = device // replicas * depth + op * group + o2
        hit = (channel == lane) & (device % replicas == 0)
        places.append(jnp.where(hit, 1.0, 0.0).astype(BF16))

    def one(step, carry):
        b, p = step // GROUP_ST, step % GROUP_ST
        sent = [
            lines[pl.ds(b * rows_of + op * GROUP_ST + p, count, stride=here * rows_of), :]
            for op in range(pairings)
        ]
        sent = jnp.concatenate(sent, 0)
        value = jnp.zeros((width, OUTCH), F32)
        for o2 in range(group):
            part = sent[:, o2 * width:(o2 + 1) * width].astype(BF16)
            value += lax.dot_general(
                part, places[o2], (((0,), (0,)), ((), ())), preferred_element_type=F32)
        value = value.reshape(slots, 2, GROUP_ST, OUTCH)
        out[b, :, :, pl.ds(pl.multiple_of(p * GROUP_ST, GROUP_ST), GROUP_ST), :] = value
        return carry

    lax.fori_loop(0, here * GROUP_ST, one, 0, unroll=8)


VMEM = pl.BlockSpec(memory_space=pltpu.VMEM)
SMEM = pl.BlockSpec(memory_space=pltpu.SMEM)
PARAMS = pltpu.CompilerParams(vmem_limit_bytes=48 * 1024 * 1024)


def from_behind(value, axis, steps):
    count = lax.axis_size(axis)
    first, last = (max(0, -steps), min(count, count - steps))
    return lax.ppermute(value, axis, [(source, source + steps) for source in range(first, last)])


def exchange_kernel(dims, shared, *refs):
    owners, pairs = dims
    devices = owners * pairs
    buffers = 2 if shared else 1
    sources, targets = refs[:buffers], refs[buffers:2 * buffers]
    send_sems, recv_sems, own_sems = refs[2 * buffers:]
    me = lax.axis_index("tm") * pairs + lax.axis_index("pair")
    barrier = pltpu.get_barrier_semaphore()

    def place_of(device):
        return (device // pairs, device % pairs)

    def greet(step, carry):
        peer = (me + step) % devices
        pl.semaphore_signal(barrier, inc=1, device_id=place_of(peer), device_id_type=pl.DeviceIdType.MESH)
        return carry

    lax.fori_loop(1, devices, greet, 0)
    pl.semaphore_wait(barrier, devices - 1)

    def piece(which, device):
        return sources[0].at[device] if which == 0 else sources[1]

    def copies(step, peer, slot):
        return [
            pltpu.make_async_remote_copy(
                src_ref=piece(which, peer), dst_ref=targets[which].at[slot],
                send_sem=send_sems.at[which, step], recv_sem=recv_sems.at[which, step],
                device_id=place_of(peer), device_id_type=pl.DeviceIdType.MESH)
            for which in range(buffers)
        ]

    def start(step, carry):
        for copy in copies(step, (me + step) % devices, me):
            copy.start()
        return carry

    lax.fori_loop(1, devices, start, 0)
    for which in range(buffers):
        own = pltpu.make_async_copy(piece(which, me), targets[which].at[me], own_sems.at[which])
        own.start()
        own.wait()

    def finish(step, carry):
        for copy in copies(step, (me + step) % devices, me):
            copy.wait_send()
        source = (me + devices - step) % devices
        for copy in copies(step, source, source):
            copy.wait_recv()
        return carry

    lax.fori_loop(1, devices, finish, 0)


def exchange(value, number, shared=None):
    owners, pairs = lax.axis_size("tm"), lax.axis_size("pair")
    devices = owners * pairs
    shapes = [jax.ShapeDtypeStruct(value.shape, value.dtype)]
    values = [value]
    if shared is not None:
        shapes.append(jax.ShapeDtypeStruct((devices,) + shared.shape, shared.dtype))
        values.append(shared)
    result = pl.pallas_call(
        functools.partial(exchange_kernel, (owners, pairs), shared is not None),
        out_shape=shapes,
        in_specs=[VMEM] * len(values),
        out_specs=[VMEM] * len(values),
        scratch_shapes=[
            pltpu.SemaphoreType.DMA((len(values), devices)),
            pltpu.SemaphoreType.DMA((len(values), devices)),
            pltpu.SemaphoreType.DMA((len(values),)),
        ],
        compiler_params=pltpu.CompilerParams(collective_id=number, has_side_effects=True),
        name="exchange",
    )(*values)
    return result if shared is not None else result[0]


def body(voltages, delays, phase_model, phase_bins, assignment):
    owners, pairs = lax.axis_size("tm"), lax.axis_size("pair")
    devices = owners * pairs
    stations, samples = voltages.shape[1], voltages.shape[2]
    frames = samples // NCHAN
    slots = assignment.shape[0]
    channel_groups = min(devices, OUTCH)
    depth = OUTCH // channel_groups
    replicas = devices // channel_groups
    group = min(2, depth)
    count = frames * stations

    first, twist, second = section_tables(stations)
    lines = voltages.reshape(2, stations, samples // LANES, LANES)
    ahead = min(DELAY_MAX, samples)
    last = DELAY_MAX - ahead
    following = from_behind(lines[:, :, :ahead // LANES], "tm", -1)
    beyond = from_behind(lines[:, :, :last // LANES], "tm", -2)

    angles = lax.dynamic_slice_in_dim(phase_model, lax.axis_index("pair") * stations, stations, 0)
    angles = angles.reshape(stations, OUTCH, QUADS, RADIX_A).transpose(2, 0, 3, 1)
    angles = angles.reshape(QUADS, stations * RADIX_A, OUTCH)
    phase = jnp.stack([jnp.cos(angles), jnp.sin(angles)])

    total_rows = (samples + DELAY_MAX) // LANES + 8
    sk = stations * RADIX_A
    spectra = pl.pallas_call(
        functools.partial(spectra_kernel, (frames, stations)),
        out_shape=jax.ShapeDtypeStruct((OUTCH, count, LANES), BF16),
        in_specs=[SMEM] + [VMEM] * 7,
        out_specs=VMEM,
        scratch_shapes=[
            pltpu.VMEM((2, stations, total_rows, LANES), F32),
            pltpu.VMEM((2 * sk, RADIX_B), BF16),
            pltpu.VMEM((frames * sk, 2 * RADIX_B), BF16),
            pltpu.VMEM((count, LANES, LANES), F32),
            pltpu.VMEM((OUTCH * count, LANES), F32),
        ],
        compiler_params=PARAMS,
        name="spectra",
    )(delays, lines, following, beyond, first, twist, second, phase)

    sent = spectra.reshape(channel_groups, depth * count, LANES)
    if replicas > 1:
        sent = jnp.repeat(sent, replicas, axis=0)
    own_small = jnp.concatenate([phase_bins, assignment])
    own_small = jnp.pad(own_small, (0, LANES - own_small.shape[0])).reshape(1, LANES)
    routed, small = exchange(sent, 0, own_small)
    small = small[:, 0, :frames + slots]
    routed = routed.reshape(owners, pairs, depth, frames, stations, LANES)

    all_bins = BINS
    bins_here = all_bins // owners
    rows_of = depth // group * GROUP_ST
    binned = pl.pallas_call(
        functools.partial(product_kernel, (owners, pairs, group, slots)),
        out_shape=jax.ShapeDtypeStruct((owners, pairs, bins_here, rows_of, LANES), BF16),
        in_specs=[SMEM, VMEM],
        out_specs=VMEM,
        scratch_shapes=[pltpu.VMEM((all_bins, depth // group, pairs * stations, LANES), F32)],
        compiler_params=PARAMS,
        name="products",
    )(small, routed)

    returned = exchange(binned.reshape(devices, bins_here, rows_of, LANES), 1)
    return pl.pallas_call(
        functools.partial(place_kernel, (replicas, depth, group)),
        out_shape=jax.ShapeDtypeStruct((bins_here, slots, 2, GROUP_ST * GROUP_ST, OUTCH), F32),
        in_specs=[VMEM],
        out_specs=VMEM,
        scratch_shapes=[pltpu.VMEM((devices * bins_here * rows_of, LANES), F32)],
        compiler_params=PARAMS,
        name="place",
    )(returned)


def solution(mesh):
    in_specs = (P(None, "pair", "tm"), P("pair", "tm"), P(), P("tm"), P("pair"))
    out_specs = P("tm", "pair", None, None, None)
    return jax.shard_map(body, mesh=mesh, in_specs=in_specs, out_specs=out_specs, check_vma=False)
```
